16 devices in a mesh: dp: 2 (over y, z), tp: 8 (over x, core).
Axes of the slice: x: 4, y: 2, z: 1, core: 2. Of those that a mesh axis runs over, the one named last changes fastest.
The devices are a block of a 4x4x8 slice.
Arguments:
- hidden: bfloat16 [6, 3840], P('dp'), parts along dimension 0
- positions: int32 [6], P('dp'), parts along dimension 0
- k_local: bfloat16 [6, 1024, 8, 256], P('dp', None, 'tp'), parts along dimension 0
- v_local: bfloat16 [6, 1024, 8, 256], P('dp', None, 'tp'), parts along dimension 0
- k_global: bfloat16 [6, 6144, 8, 256], P('dp', None, 'tp'), parts along dimension 0
- v_global: bfloat16 [6, 6144, 8, 256], P('dp', None, 'tp'), parts along dimension 0
- w_query: bfloat16 [2, 3840, 4096], P(None, None, 'tp')
- w_key: bfloat16 [2, 3840, 2048], P(None, None, 'tp')
- w_value: bfloat16 [2, 3840, 2048], P(None, None, 'tp')
- w_out: bfloat16 [2, 4096, 3840], P(None, 'tp')
- w_gate: bfloat16 [2, 3840, 15360], P(None, None, 'tp')
- w_up: bfloat16 [2, 3840, 15360], P(None, None, 'tp')
- w_down: bfloat16 [2, 15360, 3840], P(None, 'tp')
- norm_scale: float32 [2, 4, 3840], replicated
Outputs:
- output 1: bfloat16 [6, 3840], P('dp'), parts along dimension 0
- output 2: bfloat16 [6, 1024, 8, 256], P('dp', None, 'tp'), parts along dimension 0
- output 3: bfloat16 [6, 1024, 8, 256], P('dp', None, 'tp'), parts along dimension 0
- output 4: bfloat16 [6, 6144, 8, 256], P('dp', None, 'tp'), parts along dimension 0
- output 5: bfloat16 [6, 6144, 8, 256], P('dp', None, 'tp'), parts along dimension 0
There are 2 independent parts. The reference program is written for one: setup_inputs(seed, part) draws one part's arguments, and reference() takes and returns one part's arrays. A program takes and returns all parts, laid end to end along the dimension named above; an argument that names none is the same for every part.
All inputs are finite; a program needn't handle non-finite values.
Results may differ from the reference program's by a relative error of at most 0.02.
Values are sent between devices in bfloat16 or wider.
A program may use at most 768 MiB of HBM per device.

```python
import jax
import jax.numpy as jnp
from jax import lax

D = 3840
HEADS = 16
KV_HEADS = 8
HEAD = 256
FF = 15360
WINDOW = 1024
BATCH = 3
CTX = 6144

SOFT_CAP = 50.0
NORM_EPS = 1e-6
ROPE_BASE = 10000.0
NEG_FILL = -1e30


def draw_positions(pos_key):
    draw_key, row_key = jax.random.split(pos_key)
    drawn_pos = jax.random.randint(draw_key, (BATCH,), WINDOW, CTX, dtype=jnp.int32)
    top_row = jax.random.randint(row_key, (), 0, BATCH, dtype=jnp.int32)
    row_ids = jnp.arange(BATCH, dtype=jnp.int32)
    return jnp.where(row_ids == top_row, CTX - 1, drawn_pos).astype(jnp.int32)


def normal_bf16(rand_key, arr_shape, std_scale):
    return (jax.random.normal(rand_key, arr_shape, jnp.float32) * std_scale).astype(jnp.bfloat16)


def setup_inputs(seed: int = 0, part: int = 0) -> dict:
    part_key = jax.random.fold_in(jax.random.key(seed), part)
    row_keys = jax.random.split(part_key, 6)
    weight_keys = jax.random.split(jax.random.key(seed + 1), 8)
    value_gain = jnp.sqrt(jnp.array([WINDOW, CTX], dtype=jnp.float32)).reshape(2, 1, 1)
    return {
        'hidden': normal_bf16(row_keys[0], (BATCH, D), 1.0),
        'positions': draw_positions(row_keys[1]),
        'k_local': normal_bf16(row_keys[2], (BATCH, WINDOW, KV_HEADS, HEAD), 1.0),
        'v_local': normal_bf16(row_keys[3], (BATCH, WINDOW, KV_HEADS, HEAD), 1.0),
        'k_global': normal_bf16(row_keys[4], (BATCH, CTX, KV_HEADS, HEAD), 1.0),
        'v_global': normal_bf16(row_keys[5], (BATCH, CTX, KV_HEADS, HEAD), 1.0),
        'w_query': normal_bf16(weight_keys[0], (2, D, HEADS * HEAD), D ** -0.5),
        'w_key': normal_bf16(weight_keys[1], (2, D, KV_HEADS * HEAD), D ** -0.5),
        'w_value': normal_bf16(weight_keys[2], (2, D, KV_HEADS * HEAD), value_gain * D ** -0.5),
        'w_out': normal_bf16(weight_keys[3], (2, HEADS * HEAD, D), (HEADS * HEAD) ** -0.5),
        'w_gate': normal_bf16(weight_keys[4], (2, D, FF), D ** -0.5),
        'w_up': normal_bf16(weight_keys[5], (2, D, FF), D ** -0.5),
        'w_down': normal_bf16(weight_keys[6], (2, FF, D), FF ** -0.5),
        'norm_scale': jax.random.normal(weight_keys[7], (2, 4, D), jnp.float32) * 0.4,
    }


def rms_norm(values, gain_row):
    values_f32 = values.astype(jnp.float32)
    inv_rms = lax.rsqrt(jnp.mean(values_f32 * values_f32, axis=-1, keepdims=True) + NORM_EPS)
    return (values_f32 * inv_rms * (1.0 + gain_row)).astype(jnp.bfloat16)


def rotary(projected, positions):
    half_dim = HEAD // 2
    inv_freq = ROPE_BASE ** (-2.0 * jnp.arange(half_dim, dtype=jnp.float32) / HEAD)
    angles = positions.astype(jnp.float32)[:, None, None] * inv_freq
    cos_part = jnp.cos(angles)
    sin_part = jnp.sin(angles)
    first_half = projected[..., :half_dim]
    second_half = projected[..., half_dim:]
    return jnp.concatenate([first_half * cos_part - second_half * sin_part, second_half * cos_part + first_half * sin_part], axis=-1)


def attend_row(row_args):
    queries, key_rows, value_rows, key_valid = row_args
    logits = jnp.einsum('grd,ngd->grn', queries.astype(jnp.float32), key_rows.astype(jnp.float32)) * HEAD ** -0.5
    logits = SOFT_CAP * jnp.tanh(logits / SOFT_CAP)
    logits = jnp.where(key_valid[None, None, :], logits, NEG_FILL)
    attn_probs = jax.nn.softmax(logits, axis=-1).astype(jnp.bfloat16)
    mixed_heads = jnp.einsum('grn,ngd->grd', attn_probs.astype(jnp.float32), value_rows.astype(jnp.float32))
    return mixed_heads.astype(jnp.bfloat16)


def add_normed(hidden, branch_sum, gain_row):
    return (hidden.astype(jnp.float32) + rms_norm(branch_sum, gain_row).astype(jnp.float32)).astype(jnp.bfloat16)


def decoder_layer(hidden, positions, k_cache, v_cache, slot_ids, key_valid, layer_weights, gains):
    w_query, w_key, w_value, w_out, w_gate, w_up, w_down = layer_weights
    normed = rms_norm(hidden, gains[0])
    queries = jnp.dot(normed, w_query, preferred_element_type=jnp.float32).reshape(BATCH, HEADS, HEAD)
    key_new = jnp.dot(normed, w_key, preferred_element_type=jnp.float32).reshape(BATCH, KV_HEADS, HEAD)
    value_new = jnp.dot(normed, w_value, preferred_element_type=jnp.float32).astype(jnp.bfloat16).reshape(BATCH, KV_HEADS, HEAD)
    queries = rotary(queries, positions).astype(jnp.bfloat16)
    key_new = rotary(key_new, positions).astype(jnp.bfloat16)
    slot_hit = (jnp.arange(k_cache.shape[1])[None, :] == slot_ids[:, None])[:, :, None, None]
    k_cache = jnp.where(slot_hit, key_new[:, None], k_cache)
    v_cache = jnp.where(slot_hit, value_new[:, None], v_cache)
    grouped = queries.reshape(BATCH, KV_HEADS, HEADS // KV_HEADS, HEAD)
    mixed_heads = lax.map(attend_row, (grouped, k_cache, v_cache, key_valid))
    attn_sum = jnp.dot(mixed_heads.reshape(BATCH, HEADS * HEAD), w_out, preferred_element_type=jnp.float32)
    hidden = add_normed(hidden, attn_sum, gains[1])
    normed = rms_norm(hidden, gains[2])
    gate_proj = jnp.dot(normed, w_gate, preferred_element_type=jnp.float32)
    up_proj = jnp.dot(normed, w_up, preferred_element_type=jnp.float32)
    hidden_act = (jax.nn.gelu(gate_proj, approximate=True) * up_proj).astype(jnp.bfloat16)
    down_sum = jnp.dot(hidden_act, w_down, preferred_element_type=jnp.float32)
    hidden = add_normed(hidden, down_sum, gains[3])
    return hidden, k_cache, v_cache


def reference(hidden, positions, k_local, v_local, k_global, v_global, w_query, w_key, w_value, w_out, w_gate, w_up, w_down, norm_scale):
    stacks = (w_query, w_key, w_value, w_out, w_gate, w_up, w_down)
    local_valid = jnp.full((BATCH, WINDOW), True)
    global_valid = jnp.arange(CTX)[None, :] <= positions[:, None]
    hidden, k_local, v_local = decoder_layer(hidden, positions, k_local, v_local, positions % WINDOW, local_valid, tuple(stacked[0] for stacked in stacks), norm_scale[0])
    hidden, k_global, v_global = decoder_layer(hidden, positions, k_global, v_global, positions, global_valid, tuple(stacked[1] for stacked in stacks), norm_scale[1])
    return (hidden, k_local, v_local, k_global, v_global)
```

```python
import functools

import jax
import jax.numpy as jnp
from jax import lax
from jax.experimental import pallas as pl
from jax.experimental.pallas import tpu as pltpu
from jax.sharding import PartitionSpec as P

SOFT_CAP = 50.0
NORM_EPS = 1e-6
ROPE_BASE = 10000.0

TILE = 256
GATE_SLOTS = 10
GATE_BLOCK = 3
DOWN_SLOTS = 6
DOWN_COLS = 384
SEND_COLS = 768
QKV_ROWS = 768
SCORE_COLS = 1024
MESH = pl.DeviceIdType.MESH
F32 = jnp.float32
BF16 = jnp.bfloat16


def dot(lhs, rhs):
    return jnp.dot(lhs, rhs, preferred_element_type=F32)


def dot_t(lhs, rhs):
    return lax.dot_general(lhs, rhs, (((1,), (1,)), ((), ())), preferred_element_type=F32)


def pad_rows(top):
    return jnp.concatenate([top, jnp.zeros_like(top)], axis=0).astype(BF16)


def step_kernel(tp, hid, pos, kl, vl, kg, vg, wq, wk, wv, wo, wg, wu, wd, ns, out, klo, vlo, kgo, vgo, knew, vnew, hid_s, ns_s, qkv_s, wo_s, wg_s, wu_s, wd_s, x_s, a8_s, a16_s, acc_s, s_s, p_s, h_s, rb, m_sem, q_sem, c_sem, o_sem, g_sem, d_sem, s_sem, r_sem):
    rows, width = hid.shape
    head = kl.shape[-1]
    half = head // 2
    ff = wg.shape[-1]
    layers = wq.shape[0]
    q_cols = wq.shape[-1]
    windows = (kl.shape[1], kg.shape[1])
    n_gate = width // TILE
    n_down = width // DOWN_COLS
    n_send = width // SEND_COLS
    n_qkv = width // QKV_ROWS
    me = lax.axis_index('tp')

    barrier = pltpu.get_barrier_semaphore()
    for d in range(1, tp):
        pl.semaphore_signal(barrier, inc=1, device_id={'tp': lax.rem(me + d, tp)}, device_id_type=MESH)

    def qkv_copies(l, c):
        r = pl.ds(c * QKV_ROWS, QKV_ROWS)
        return [
            pltpu.make_async_copy(wq.at[l, r, :], qkv_s.at[r, pl.ds(0, q_cols)], q_sem.at[0, c]),
            pltpu.make_async_copy(wk.at[l, r, :], qkv_s.at[r, pl.ds(q_cols, head)], q_sem.at[1, c]),
            pltpu.make_async_copy(wv.at[l, r, :], qkv_s.at[r, pl.ds(q_cols + head, head)], q_sem.at[2, c]),
        ]

    def cache_copy(l, i, b):
        src = ((kl, vl), (kg, vg))[l][i]
        dst = ((klo, vlo), (kgo, vgo))[l][i]
        return pltpu.make_async_copy(src.at[b], dst.at[b], c_sem.at[l, i, b])

    def out_copy(l):
        return pltpu.make_async_copy(wo.at[l], wo_s, o_sem)

    def gate_copies(l, c):
        slot = c % GATE_SLOTS
        r = pl.ds(c * TILE, TILE)
        return [
            pltpu.make_async_copy(wg.at[l, r, :], wg_s.at[slot], g_sem.at[0, slot]),
            pltpu.make_async_copy(wu.at[l, r, :], wu_s.at[slot], g_sem.at[1, slot]),
        ]

    n_quad = n_down - DOWN_SLOTS

    def down_slot(j):
        if j < n_quad:
            return qkv_s.at[pl.ds((j // 2) * ff, ff), pl.ds((j % 2) * DOWN_COLS, DOWN_COLS)]
        return wd_s.at[j - n_quad]

    def down_copy(l, j):
        return pltpu.make_async_copy(wd.at[l, :, pl.ds(j * DOWN_COLS, DOWN_COLS)], down_slot(j), d_sem.at[j])

    hid_copy = pltpu.make_async_copy(hid, hid_s, m_sem.at[0])
    ns_copy = pltpu.make_async_copy(ns, ns_s, m_sem.at[1])
    hid_copy.start()
    ns_copy.start()
    for c in range(n_qkv):
        for cp in qkv_copies(0, c):
            cp.start()
    for i in range(2):
        for b in range(rows):
            cache_copy(0, i, b).start()
    out_copy(0).start()
    for c in range(GATE_SLOTS):
        for cp in gate_copies(0, c):
            cp.start()
    for b in range(rows - 1):
        cache_copy(1, 0, b).start()

    row8 = lax.broadcasted_iota(jnp.int32, (8, half), 0)
    pos8 = jnp.zeros((8, half), jnp.int32)
    for b in range(rows):
        pos8 = jnp.where(row8 == b, pos[b], pos8)
    lane = lax.broadcasted_iota(jnp.int32, (8, half), 1).astype(F32)
    angles = pos8.astype(F32) * jnp.exp(lane * (-2.0 / head * 9.210340371976184))
    cos_part = jnp.cos(angles)
    sin_part = jnp.sin(angles)

    def rotary(full):
        first, second = full[:, :half], full[:, half:]
        return jnp.concatenate([first * cos_part - second * sin_part, second * cos_part + first * sin_part], axis=-1)

    def blocks():
        return [slice(j * SEND_COLS, (j + 1) * SEND_COLS) for j in range(n_send)]

    def inv_rms(parts):
        total = sum(jnp.sum(p * p, axis=-1, keepdims=True) for p in parts)
        return lax.rsqrt(total * (1.0 / width) + NORM_EPS)

    def scaled(parts, l, i):
        inv = inv_rms(parts)
        return [(p * inv * (1.0 + ns_s[l, i : i + 1, cols])).astype(BF16) for p, cols in zip(parts, blocks())]

    def set_operand(parts):
        for p, cols in zip(parts, blocks()):
            a8_s[0:rows, cols] = p.astype(F32)
        for c in range(n_gate):
            cols = slice(c * TILE, (c + 1) * TILE)
            a16_s[:, cols] = pad_rows(a8_s[:, cols])

    def sends(ar, j):
        return [
            pltpu.make_async_remote_copy(
                src_ref=rb.at[ar, me, j],
                dst_ref=rb.at[ar, me, j],
                send_sem=s_sem.at[ar, d],
                recv_sem=r_sem.at[ar, me],
                device_id={'tp': lax.rem(me + d, tp)},
                device_id_type=MESH,
            )
            for d in range(1, tp)
        ]

    def whole(ar, d):
        src = lax.rem(me + d, tp)
        return pltpu.make_async_remote_copy(
            src_ref=rb.at[ar, src],
            dst_ref=rb.at[ar, src],
            send_sem=s_sem.at[ar, d],
            recv_sem=r_sem.at[ar, src],
            device_id={'tp': src},
            device_id_type=MESH,
        )

    def received(ar):
        for d in range(1, tp):
            whole(ar, d).wait_recv()
        parts = []
        for j in range(n_send):
            total = rb[ar, 0, j].astype(F32)
            for s in range(1, tp):
                total = total + rb[ar, s, j].astype(F32)
            parts.append(total)
        return parts

    def attend(l, q8, k8, v8):
        k_ref, v_ref = ((klo, vlo), (kgo, vgo))[l]
        n = windows[l]
        cols = min(SCORE_COLS, n)
        row16 = lax.broadcasted_iota(jnp.int32, (16, 1), 0)
        row16 = jnp.where(row16 >= 8, row16 - 8, row16)
        pos16 = jnp.zeros((16, 1), jnp.int32)
        for b in range(rows):
            pos16 = jnp.where(row16 == b, pos[b], pos16)
        slot16 = lax.rem(pos16, n) if l == 0 else pos16
        q16 = jnp.concatenate(q8, axis=0)
        s_new = jnp.concatenate([jnp.sum(q * k8, axis=-1, keepdims=True) for q in q8], axis=0)
        scale = head**-0.5 / SOFT_CAP

        def weight(s):
            return jnp.exp(SOFT_CAP * jnp.tanh(s * scale))

        q_row = [jnp.where(row16 == b, q16, 0.0).astype(BF16) for b in range(rows)]
        for b in range(rows):
            cache_copy(l, 0, b).wait()
            for t in range(n // cols):
                span = slice(t * cols, (t + 1) * cols)
                s = dot_t(q_row[b], k_ref[b, span, :])
                if b:
                    s = s + s_s[:, span]
                s_s[:, span] = s
        total = jnp.zeros((16, 1), F32)
        for t in range(n // cols):
            span = slice(t * cols, (t + 1) * cols)
            slot_ids = lax.broadcasted_iota(jnp.int32, (16, cols), 1) + t * cols
            e = weight(jnp.where(slot_ids == slot16, s_new, s_s[:, span]))
            if l:
                e = jnp.where(slot_ids <= pos16, e, 0.0)
            s_s[:, span] = e
            total = total + jnp.sum(e, axis=-1, keepdims=True)
        inv = 1.0 / total
        for t in range(n // cols):
            span = slice(t * cols, (t + 1) * cols)
            slot_ids = lax.broadcasted_iota(jnp.int32, (16, cols), 1) + t * cols
            p_s[:, span] = jnp.where(slot_ids == slot16, 0.0, s_s[:, span] * inv).astype(BF16)
        p_new = (weight(s_new) * inv).astype(BF16).astype(F32)
        mixed = p_new * jnp.concatenate([v8, v8], axis=0)
        for b in range(rows):
            cache_copy(l, 1, b).wait()
            mixed = mixed + jnp.where(row16 == b, dot(p_s[:, 0:n], v_ref[b]), 0.0)
        return jnp.concatenate([mixed[:8], mixed[8:]], axis=-1)

    a8_s[...] = jnp.zeros_like(a8_s)
    hid_copy.wait()
    ns_copy.wait()
    x = [hid_s[:, cols].astype(F32) for cols in blocks()]
    for l in range(layers):
        if l:
            x = [x_s[j] for j in range(n_send)]
        set_operand(scaled(x, l, 0))
        qkv = None
        for c in range(n_qkv):
            for cp in qkv_copies(l, c):
                cp.wait()
            r = slice(c * QKV_ROWS, (c + 1) * QKV_ROWS)
            part = dot(a16_s[:, r], qkv_s[r, :])[:8]
            qkv = part if qkv is None else qkv + part
        q8 = [rotary(qkv[:, h * head : (h + 1) * head]).astype(BF16).astype(F32) for h in range(q_cols // head)]
        k8 = rotary(qkv[:, q_cols : q_cols + head]).astype(BF16).astype(F32)
        v8 = qkv[:, q_cols + head : q_cols + 2 * head].astype(BF16).astype(F32)
        knew[l] = k8
        vnew[l] = v8
        mixed = pad_rows(attend(l, q8, k8, v8))

        out_copy(l).wait()
        ar = 2 * l
        if l == 0:
            pl.semaphore_wait(barrier, tp - 1)
        for j, cols in enumerate(blocks()):
            rb[ar, me, j] = dot(mixed, wo_s[:, cols])[:rows].astype(BF16)
            for cp in sends(ar, j):
                cp.start()
        if l == 0:
            x = [hid_s[:, cols].astype(F32) for cols in blocks()]
        else:
            x = [x_s[j] for j in range(n_send)]
        x = [(p + q.astype(F32)).astype(BF16).astype(F32) for p, q in zip(x, scaled(received(ar), l, 1))]
        for j in range(n_send):
            x_s[j] = x[j]
        set_operand(scaled(x, l, 2))

        for c0 in range(0, n_gate, GATE_BLOCK):
            chunks = range(c0, min(c0 + GATE_BLOCK, n_gate))
            for c in chunks:
                for cp in gate_copies(l, c):
                    cp.wait()
            for i, buf in enumerate((wg_s, wu_s)):
                part = sum(dot(a16_s[:, c * TILE : (c + 1) * TILE], buf[c % GATE_SLOTS]) for c in chunks)[:8]
                acc_s[i] = part if c0 == 0 else acc_s[i] + part
            for c in chunks:
                if c + GATE_SLOTS < n_gate:
                    for cp in gate_copies(l, c + GATE_SLOTS):
                        cp.start()
                if c + GATE_SLOTS == n_gate - 1:
                    for j in range(n_down):
                        down_copy(l, j).start()
                    if l == 0:
                        cache_copy(1, 0, rows - 1).start()
        h_s[...] = pad_rows(jax.nn.gelu(acc_s[0], approximate=True) * acc_s[1])

        ar = 2 * l + 1
        per_send = SEND_COLS // DOWN_COLS
        for j in range(n_send):
            chunks = range(j * per_send, (j + 1) * per_send)
            for c in chunks:
                down_copy(l, c).wait()
            for i, c in enumerate(chunks):
                rb[ar, me, j, :, i * DOWN_COLS : (i + 1) * DOWN_COLS] = dot(h_s[...], down_slot(c)[...])[:rows].astype(BF16)
            for cp in sends(ar, j):
                cp.start()
            if l == 0 and (j + 1) * per_send == n_quad:
                for c in range(n_qkv):
                    for cp in qkv_copies(1, c):
                        cp.start()
                for b in range(rows):
                    cache_copy(1, 1, b).start()
                out_copy(1).start()
                for c in range(GATE_SLOTS):
                    for cp in gate_copies(1, c):
                        cp.start()
        x = [x_s[j] for j in range(n_send)]
        x = [(p + q.astype(F32)).astype(BF16) for p, q in zip(x, scaled(received(ar), l, 3))]
        if l + 1 < layers:
            for j in range(n_send):
                x_s[j] = x[j].astype(F32)
        else:
            for j, cols in enumerate(blocks()):
                out[:, cols] = x[j]
    for ar in range(2 * layers):
        for d in range(1, tp):
            whole(ar, d).wait_send()


def store_kernel(pos, knew, vnew, kl, vl, kg, vg, klo, vlo, kgo, vgo, kl_s, vl_s, kg_s, vg_s, sem):
    rows = kl.shape[0]
    copies = []
    for l, (k_ref, v_ref, k_out, v_out) in enumerate(((kl_s, vl_s, klo, vlo), (kg_s, vg_s, kgo, vgo))):
        window = k_ref.shape[1]
        for i, (new, ref, dst) in enumerate(((knew, k_ref, k_out), (vnew, v_ref, v_out))):
            for b in range(rows):
                slot = lax.rem(pos[b], window)
                base = pl.multiple_of((slot // 16) * 16, 16)
                tile = ref[b, pl.ds(base, 16), :].astype(F32)
                hit = lax.broadcasted_iota(jnp.int32, tile.shape, 0) == slot - base
                ref[b, pl.ds(base, 16), :] = jnp.where(hit, new[l, b : b + 1, :], tile).astype(BF16)
                cp = pltpu.make_async_copy(ref.at[b], dst.at[b], sem.at[l, i, b])
                cp.start()
                copies.append(cp)
    for cp in copies:
        cp.wait()


def decode_step(tp, hidden, positions, k_local, v_local, k_global, v_global, w_query, w_key, w_value, w_out, w_gate, w_up, w_down, norm_scale):
    rows, width = hidden.shape
    head = k_local.shape[-1]
    layers = w_query.shape[0]
    ff = w_gate.shape[-1]
    caches = [c.reshape(rows, c.shape[1], head) for c in (k_local, v_local, k_global, v_global)]
    window = k_global.shape[1]
    hbm = lambda v: pltpu.with_memory_space_constraint(v, pltpu.HBM)
    any_spec = pl.BlockSpec(memory_space=pl.ANY)
    vmem_spec = pl.BlockSpec(memory_space=pltpu.VMEM)
    smem_spec = pl.BlockSpec(memory_space=pltpu.SMEM)
    dma = pltpu.SemaphoreType.DMA
    n_send = width // SEND_COLS
    big = [hbm(v) for v in (*caches, w_query, w_key, w_value, w_out, w_gate, w_up, w_down)]
    cache_shapes = [pltpu.VMEM(c.shape, BF16) for c in caches]
    new_shape = pltpu.VMEM((layers, 8, head), F32)
    out, klo, vlo, kgo, vgo, knew, vnew = pl.pallas_call(
        functools.partial(step_kernel, tp),
        out_shape=(jax.ShapeDtypeStruct((rows, width), BF16), *cache_shapes, new_shape, new_shape),
        in_specs=[any_spec, smem_spec] + [any_spec] * 12,
        out_specs=(vmem_spec,) * 7,
        scratch_shapes=[
            pltpu.VMEM((rows, width), BF16),
            pltpu.VMEM(norm_scale.shape, F32),
            pltpu.VMEM((width, w_query.shape[-1] + 2 * head), BF16),
            pltpu.VMEM(w_out.shape[1:], BF16),
            pltpu.VMEM((GATE_SLOTS, TILE, ff), BF16),
            pltpu.VMEM((GATE_SLOTS, TILE, ff), BF16),
            pltpu.VMEM((DOWN_SLOTS, ff, DOWN_COLS), BF16),
            pltpu.VMEM((n_send, rows, SEND_COLS), F32),
            pltpu.VMEM((8, width), F32),
            pltpu.VMEM((16, width), BF16),
            pltpu.VMEM((2, 8, ff), F32),
            pltpu.VMEM((16, window), F32),
            pltpu.VMEM((16, window), BF16),
            pltpu.VMEM((16, ff), BF16),
            pltpu.VMEM((2 * layers, tp, n_send, rows, SEND_COLS), BF16),
            dma((2,)),
            dma((3, width // QKV_ROWS)),
            dma((2, 2, rows)),
            dma(()),
            dma((2, GATE_SLOTS)),
            dma((width // DOWN_COLS,)),
            dma((2 * layers, tp)),
            dma((2 * layers, tp)),
        ],
        compiler_params=pltpu.CompilerParams(vmem_limit_bytes=42 * 2**20, collective_id=0, has_side_effects=True),
        name='decode',
    )(hbm(hidden), positions, *big, hbm(norm_scale))
    stored = pl.pallas_call(
        store_kernel,
        out_shape=tuple(jax.ShapeDtypeStruct(c.shape, BF16) for c in caches) + tuple(cache_shapes),
        in_specs=[smem_spec] + [vmem_spec] * 6,
        out_specs=(any_spec,) * 4 + (vmem_spec,) * 4,
        input_output_aliases={3: 4, 4: 5, 5: 6, 6: 7},
        scratch_shapes=[dma((2, 2, rows))],
        compiler_params=pltpu.CompilerParams(vmem_limit_bytes=2 * 2**20),
        name='store',
    )(positions, knew, vnew, klo, vlo, kgo, vgo)
    return (out, *(s.reshape(c.shape) for s, c in zip(stored[:4], (k_local, v_local, k_global, v_global))))


def solution(mesh):
    row_spec = P('dp', None)
    cache_spec = P('dp', None, 'tp', None)
    col_split = P(None, None, 'tp')
    row_split = P(None, 'tp', None)
    in_specs = (row_spec, P('dp'), cache_spec, cache_spec, cache_spec, cache_spec, col_split, col_split, col_split, row_split, col_split, col_split, row_split, P())
    out_specs = (row_spec, cache_spec, cache_spec, cache_spec, cache_spec)
    return jax.shard_map(functools.partial(decode_step, mesh.shape['tp']), mesh=mesh, in_specs=in_specs, out_specs=out_specs, check_vma=False)
```
